32 devices in a mesh: dp: 8 (over z, y), tensor: 4 (over x, core).
Axes of the slice: x: 2, y: 2, z: 4, core: 2. Of those that a mesh axis runs over, the one named last changes fastest.
Arguments:
- tokens: bfloat16 [32768, 1024], P(('dp', 'tensor')), may hold values from -6 to 6
- segments: int32 [64, 512], P(('dp', 'tensor')), may hold values from 0 to 1, as said below
- lengths: int32 [64], P(('dp', 'tensor')), may hold values from 128 to 512, as said below
- type_table: bfloat16 [2, 1024], replicated, may hold values from -3 to 3
- attn_weight: bfloat16 [3145728], P(('dp', 'tensor')), may hold values from -0.1875 to 0.1875
- out_weight: bfloat16 [1048576], P(('dp', 'tensor')), may hold values from -0.75 to 0.75
- ffn_in_weight: bfloat16 [1024, 4096], P('dp', 'tensor'), may hold values from -0.1875 to 0.1875
- ffn_out_weight: bfloat16 [4096, 1024], P('tensor', 'dp'), may hold values from -0.125 to 0.125
- attn_bias: bfloat16 [3, 1024], replicated, may hold values from -3 to 3
- ffn_bias_in: bfloat16 [4096], replicated, may hold values from -3 to 3
- ffn_bias_out: bfloat16 [1024], replicated, may hold values from -3 to 3
- norm_gain: bfloat16 [2, 1024], replicated, may hold values from 0.099609375 to 1.8984375
- norm_shift: bfloat16 [2, 1024], replicated, may hold values from -3 to 3
- cotangent: bfloat16 [32768, 1024], P(('dp', 'tensor')), may hold values from -6 to 6
Outputs:
- output: bfloat16 [32768, 1024], P(('dp', 'tensor'))
- grad_input: bfloat16 [32768, 1024], P(('dp', 'tensor'))
- attn_bias_grad: float32 [3, 1024], replicated
- ffn_bias_in_grad: float32 [4096], replicated
- ffn_bias_out_grad: float32 [1024], replicated
- norm_gain_grad: float32 [2, 1024], replicated
- norm_shift_grad: float32 [2, 1024], replicated
The draws below stay inside these ranges and needn't reach their ends.
Inputs may be any that keep to these rules, and one draw needn't show every extreme that they name: `lengths`: the valid tokens of a sequence are its first ones; in every draw some sequence has all 512 valid. `segments`: segment id 0 up to and including a separator at position 1 to length - 2, 1 after it up to the sequence's length, 0 on padding.
All inputs are finite; a program needn't handle non-finite values.
Results may differ from the reference program's by a relative error of at most 0.015.
Values may be sent and summed in bfloat16 or wider, within the bound.
A program may use at most 192 MiB of HBM per device.

```python
import math
import jax
import jax.numpy as jnp
from jax import lax

D = 1024
HEADS = 16
HEAD = 64
FF = 4096
SEQ = 512
TOKENS = 32768


def shared_rows(key):
    seq_count = TOKENS // SEQ
    seq_lengths = jax.random.randint(jax.random.fold_in(key, 11), (seq_count,), SEQ // 4, SEQ + 1)
    seq_lengths = seq_lengths.at[0].set(SEQ)
    separators = jax.random.randint(jax.random.fold_in(key, 12), (seq_count,), 1, seq_lengths - 1)
    return (seq_lengths.astype(jnp.int32), separators.astype(jnp.int32))


def draw_lengths(key, part):
    return shared_rows(key)[0]


def draw_segments(key, part):
    seq_lengths, separators = shared_rows(key)
    position = jnp.arange(SEQ, dtype=jnp.int32)[None, :]
    inside = (position > separators[:, None]) & (position < seq_lengths[:, None])
    return jnp.where(inside, 1, 0).astype(jnp.int32)


def levels(rng, dims, shards, least, high):
    gain = 1.0
    for dim, parts in shards:
        steps = jax.random.uniform(jax.random.fold_in(jax.random.fold_in(rng, 6), dim), (parts,), jnp.float32, least / len(shards), high / len(shards))
        gain = gain * jnp.repeat(jnp.exp(steps), dims[dim] // parts).reshape((-1,) + (1,) * (len(dims) - 1 - dim))
    return gain


def noise(own_key, shape, scale, limit, cuts=(), kind=jnp.bfloat16):
    drawn = scale * jax.random.normal(own_key, shape, jnp.float32)
    if cuts:
        drawn = drawn * levels(own_key, shape, cuts, -0.22, 0.18)
    return jnp.clip(drawn, -limit, limit).astype(kind)


def setup_inputs(seed: int = 0) -> dict:
    seeds = jax.random.split(jax.random.key(seed), 15)
    return {
        "tokens": noise(seeds[0], (TOKENS, D), 1.0, 6.0, ((0, 32),)),
        "segments": draw_segments(jax.random.fold_in(seeds[14], 71), 0),
        "lengths": draw_lengths(jax.random.fold_in(seeds[14], 71), 0),
        "type_table": noise(seeds[3], (2, D), 0.5, 3.0),
        "attn_weight": noise(seeds[4], (3 * D * D,), D ** -0.5, 0.1875, ((0, 32),)),
        "out_weight": noise(seeds[5], (D * D,), (D // 16) ** -0.5, 0.75, ((0, 32),)),
        "ffn_in_weight": noise(seeds[6], (D, FF), D ** -0.5, 0.1875, ((0, 8), (1, 4))),
        "ffn_out_weight": noise(seeds[7], (FF, D), (FF // 2) ** -0.5, 0.125, ((0, 4), (1, 8))),
        "attn_bias": noise(seeds[8], (3, D), 0.5, 3.0),
        "ffn_bias_in": noise(seeds[9], (FF,), 0.5, 3.0),
        "ffn_bias_out": noise(seeds[10], (D,), 0.5, 3.0),
        "norm_gain": jnp.clip(1.0 + 0.18 * jax.random.normal(seeds[11], (2, D), jnp.float32), 0.099609375, 1.8984375).astype(jnp.bfloat16),
        "norm_shift": noise(seeds[12], (2, D), 0.5, 3.0),
        "cotangent": noise(seeds[13], (TOKENS, D), 1.0, 6.0, ((0, 32),)),
    }


@jax.custom_vjp
def low(v):
    return lax.optimization_barrier(v.astype(jnp.bfloat16)).astype(jnp.float32)

@jax.custom_vjp
def low_back(v):
    return v

def low_keep(v):
    return (low(v), None)

def low_pass(kept, grad):
    return (grad,)

def back_keep(v):
    return (v, None)

def back_low(kept, grad):
    return (low(grad),)
low.defvjp(low_keep, low_pass)
low_back.defvjp(back_keep, back_low)

def matmul(left_side, right_side):
    return jnp.dot(left_side, right_side, precision=lax.Precision.HIGHEST, preferred_element_type=jnp.float32)

def layer_norm(residual, gain_row, shift_row):
    row_mean = lax.optimization_barrier(jnp.mean(residual, axis=-1, keepdims=True))
    centered = residual - row_mean
    variance = lax.optimization_barrier(jnp.mean(centered * centered, axis=-1, keepdims=True))
    return centered * lax.rsqrt(variance + 1e-12) * gain_row + shift_row

def forward(tokens, segments, lengths, type_table, projections, out_proj, w_first, w_second, attn_bias, bias_in, bias_out, norm_gain, norm_shift):
    seq_count = lengths.shape[0]
    type_rows = jnp.where((segments.reshape(-1) == 1)[:, None], type_table[1][None, :], type_table[0][None, :])
    block_input = tokens + type_rows
    lowered = low(block_input)
    queries = low_back(low(matmul(lowered, projections[0]) + attn_bias[0]))
    key_rows = low_back(low(matmul(lowered, projections[1])))
    value_rows = low_back(low(matmul(lowered, projections[2]) + attn_bias[1]))

    def to_heads(row_block):
        return row_block.reshape(seq_count, SEQ, HEADS, HEAD)
    score_scale = 1.0 / math.sqrt(HEAD)
    scores = jnp.einsum('bqhd,bkhd->bhqk', to_heads(queries), to_heads(key_rows), precision=lax.Precision.HIGHEST) * score_scale
    key_valid = jnp.arange(SEQ)[None, :] < lengths[:, None]
    masked = jnp.where(key_valid[:, None, None, :], low_back(scores), -1000000000.0)
    attn_prob = low(jax.nn.softmax(masked, axis=-1))
    context = jnp.einsum('bhqk,bkhd->bqhd', attn_prob, to_heads(value_rows), precision=lax.Precision.HIGHEST).reshape(seq_count * SEQ, D)
    context = low_back(low(context))
    attn_out = low_back(matmul(context, out_proj) + attn_bias[2])
    middle = layer_norm(block_input + attn_out, norm_gain[0], norm_shift[0])
    preact = low_back(matmul(low(middle), w_first) + bias_in)
    hidden = low(jax.nn.gelu(preact, approximate=False))
    ffn_out = low_back(matmul(hidden, w_second) + bias_out)
    return layer_norm(middle + ffn_out, norm_gain[1], norm_shift[1])

def reference(tokens, segments, lengths, type_table, attn_weight, out_weight, ffn_in_weight, ffn_out_weight, attn_bias, ffn_bias_in, ffn_bias_out, norm_gain, norm_shift, cotangent):
    projections = attn_weight.astype(jnp.float32).reshape(3, D, D)
    out_proj = out_weight.astype(jnp.float32).reshape(D, D)
    w_first = ffn_in_weight.astype(jnp.float32)
    w_second = ffn_out_weight.astype(jnp.float32)
    table_rows = type_table.astype(jnp.float32)
    params = (attn_bias.astype(jnp.float32), ffn_bias_in.astype(jnp.float32), ffn_bias_out.astype(jnp.float32), norm_gain.astype(jnp.float32), norm_shift.astype(jnp.float32))
    seq_total = lengths.shape[0]
    group = 8 if seq_total % 8 == 0 else 1
    blocks = seq_total // group
    row_in = tokens.astype(jnp.float32).reshape(blocks, group * SEQ, D)
    seg_in = segments.reshape(blocks, group, SEQ)
    len_in = lengths.reshape(blocks, group)
    cot_in = cotangent.astype(jnp.float32).reshape(blocks, group * SEQ, D)

    def one_block(totals, inputs_now):
        row_block, seg_block, len_block, cot_block = inputs_now

        def local_pass(rows_f, bias_attn, bias_first, bias_second, gain_rows, shift_rows):
            return forward(rows_f, seg_block, len_block, table_rows, projections, out_proj, w_first, w_second, bias_attn, bias_first, bias_second, gain_rows, shift_rows)
        result, pullback = jax.vjp(local_pass, row_block, *params)
        gradients = pullback(cot_block)
        totals = jax.tree.map(jnp.add, totals, tuple(gradients[1:]))
        return (totals, (result.astype(jnp.bfloat16), gradients[0].astype(jnp.bfloat16)))
    zeros = tuple((jnp.zeros(p.shape, jnp.float32) for p in params))
    totals, (outputs, grad_rows) = lax.scan(one_block, zeros, (row_in, seg_in, len_in, cot_in))
    return (outputs.reshape(TOKENS, D), grad_rows.reshape(TOKENS, D), totals[0], totals[1], totals[2], totals[3], totals[4])
```

```python
import functools, math
import jax, jax.numpy as jnp
from jax import lax
from jax.sharding import PartitionSpec as P
from jax.experimental import pallas as pl
from jax.experimental.pallas import tpu as pltpu
MESH = pl.DeviceIdType.MESH

class Gather:
    def __init__(self, groups, sems):
        dp = lax.axis_index("dp"); tn = lax.axis_index("tensor")
        self.z, self.y = dp // 2, dp % 2
        self.x, self.c = tn // 2, tn % 2
        self.inner = (self.z + 1) // 2 % 2
        self.groups = groups
        self.zs, self.zr, self.xs, self.xr, self.ys, self.yr, self.hs, self.hr, self.ds, self.dr, self.loc = sems
        self.todo = []

    def zz(self, e):
        z = self.z
        return [z, z + 1 - 2 * (z % 2), 2 - z // 2, 3 * (1 - z // 2)][e]

    def dev(self, z, y, x, c):
        return (z * 2 + y, x * 2 + c)

    def copy(self, src, dst, ss, rs, dev):
        return pltpu.make_async_remote_copy(src_ref=src, dst_ref=dst, send_sem=ss, recv_sem=rs, device_id=dev, device_id_type=MESH)

    def barrier(self):
        b = pltpu.get_barrier_semaphore()
        z, y, x, c = self.z, self.y, self.x, self.c
        for d in ((z, y, x, 1 - c), (z, y, 1 - x, c), (z, 1 - y, x, c), (self.zz(1), y, x, c)):
            pl.semaphore_signal(b, inc=1, device_id=self.dev(*d), device_id_type=MESH)
        @pl.when(self.inner == 1)
        def _():
            pl.semaphore_signal(b, inc=1, device_id=self.dev(3 - z, y, x, c), device_id_type=MESH)
            pl.semaphore_wait(b, 5)
        @pl.when(self.inner == 0)
        def _():
            pl.semaphore_wait(b, 4)

    def zcopy(self, g, e, k, pair):
        z, y, x, c = self.z, self.y, self.x, self.c
        G = self.groups[g]; zp = self.zz(e)
        view = G["dst"](zp, y, x, c)
        src = G["src"] if e == 0 else view
        to = self.zz(1) if pair else 3 - z
        return self.copy(src, view, self.zs.at[g, k], self.zr.at[g, zp], self.dev(to, y, x, c))

    def zrecv(self, g, e):
        z, y, x, c = self.z, self.y, self.x, self.c
        zp = self.zz(e); view = self.groups[g]["dst"](zp, y, x, c)
        return self.copy(view, view, self.zs.at[g, 0], self.zr.at[g, zp], self.dev(self.zz(1), y, x, c))

    def ncopy(self, g, e, ax):
        z, y, x, c = self.z, self.y, self.x, self.c
        G = self.groups[g]; zp = self.zz(e)
        view = G["dst"](zp, y, x, c)
        src = G["src"] if e == 0 else view
        S, R = (self.xs, self.xr) if ax == "x" else (self.ys, self.yr)
        to = self.dev(z, y, 1 - x, c) if ax == "x" else self.dev(z, 1 - y, x, c)
        return self.copy(src, view, S.at[g, e], R.at[g, e], to)

    def nrecv(self, g, e, ax):
        z, y, x, c = self.z, self.y, self.x, self.c
        view = self.groups[g]["dst"](self.zz(e), y, 1 - x, c) if ax == "x" else self.groups[g]["dst"](self.zz(e), 1 - y, x, c)
        S, R = (self.xs, self.xr) if ax == "x" else (self.ys, self.yr)
        return self.copy(view, view, S.at[g, e], R.at[g, e], self.dev(z, y, x, 1 - c))

    def hcopy(self, g, e, h):
        z, y, x, c = self.z, self.y, self.x, self.c
        G = self.groups[g]; zp = self.zz(e)
        full = G["dst"](zp, 1 - y, x, c) if h == 0 else G["dst"](zp, y, 1 - x, c)
        v = G["half"](full, h)
        to = self.dev(z, y, 1 - x, c) if h == 0 else self.dev(z, 1 - y, x, c)
        return self.copy(v, v, self.hs.at[g, e, h], self.hr.at[g, e, h], to)

    def hrecv(self, g, e, h):
        z, y, x, c = self.z, self.y, self.x, self.c
        G = self.groups[g]
        v = G["half"](G["dst"](self.zz(e), 1 - y, 1 - x, c), h)
        return self.copy(v, v, self.hs.at[g, e, h], self.hr.at[g, e, h], self.dev(z, y, x, 1 - c))

    def dcopy(self, g, e, k, recv=False):
        z, y, x, c = self.z, self.y, self.x, self.c
        G = self.groups[g]; zp = self.zz(e)
        cc = 1 - c if recv else c
        if k == 0: v = G["dst"](zp, y, x, cc)
        elif k == 1: v = G["dst"](zp, y, 1 - x, cc)
        elif k == 2: v = G["dst"](zp, 1 - y, x, cc)
        else: v = G["half"](G["dst"](zp, 1 - y, 1 - x, cc), k - 3)
        src = G["src"] if (e == 0 and k == 0 and not recv) else v
        return self.copy(src, v, self.ds.at[g, e, k], self.dr.at[g, e, k], self.dev(z, y, x, 1 - c))

    def own(self, g):
        G = self.groups[g]
        self.zcopy(g, 0, 0, True).start()
        @pl.when(self.inner == 1)
        def _(): self.zcopy(g, 0, 1, False).start()
        self.ncopy(g, 0, "x").start(); self.ncopy(g, 0, "y").start()
        pltpu.make_async_copy(G["src"], G["dst"](self.z, self.y, self.x, self.c), self.loc.at[g]).start()
        self.dcopy(g, 0, 0).start()

    def avail(self, g, e):
        self.zrecv(g, e).wait_recv()
        @pl.when(self.inner == 1)
        def _(): self.zcopy(g, e, e + 1, e != 1).start()
        self.ncopy(g, e, "x").start(); self.ncopy(g, e, "y").start()
        self.dcopy(g, e, 0).start()

    def near(self, g, e):
        self.nrecv(g, e, "x").wait_recv()
        self.hcopy(g, e, 1).start()
        self.dcopy(g, e, 1).start()
        self.nrecv(g, e, "y").wait_recv()
        self.hcopy(g, e, 0).start()
        self.dcopy(g, e, 2).start()

    def opp(self, g, e):
        for h in (0, 1):
            self.hrecv(g, e, h).wait_recv()
            self.dcopy(g, e, 3 + h).start()

    def partner(self, g, e):
        for k in range(5): self.dcopy(g, e, k, recv=True).wait_recv()

    def local(self, g):
        G = self.groups[g]
        pltpu.make_async_copy(G["src"], G["dst"](self.z, self.y, self.x, self.c), self.loc.at[g]).wait()

    def sent(self, g):
        self.zcopy(g, 0, 0, True).wait_send()
        @pl.when(self.inner == 1)
        def _():
            self.zcopy(g, 0, 1, False).wait_send()
            for e in (1, 2, 3): self.zcopy(g, e, e + 1, e != 1).wait_send()
        for e in range(4):
            self.ncopy(g, e, "x").wait_send(); self.ncopy(g, e, "y").wait_send()
            for h in (0, 1): self.hcopy(g, e, h).wait_send()
            for k in range(5): self.dcopy(g, e, k).wait_send()

    def steps(self, order):
        one = [("own", 0), ("avail", 1), ("near", 0), ("avail", 2), ("near", 1), ("opp", 0), ("avail", 3), ("near", 2), ("opp", 1), ("near", 3), ("opp", 2), ("opp", 3)]
        return one

def sem_shapes(n):
    D = pltpu.SemaphoreType.DMA
    return [D((n, 5)), D((n, 4)), D((n, 4)), D((n, 4)), D((n, 4)), D((n, 4)), D((n, 4, 2)), D((n, 4, 2)), D((n, 4, 5)), D((n, 4, 5)), D((n,))]

def make_groups(qkv, out, w1, w2, gq, go, g1, g2):
    lin = lambda z, y, x, c: ((z * 2 + y) * 2 + x) * 2 + c
    def rows(ref, n):
        return lambda z, y, x, c: ref.at[pl.ds(pl.multiple_of(lin(z, y, x, c) * n, n), n), :]
    def hrows(n):
        return lambda v, h: v.at[pl.ds(h * n, n), :]
    return [
        dict(src=qkv, dst=rows(gq, 96), half=hrows(48)),
        dict(src=out, dst=rows(go, 32), half=hrows(16)),
        dict(src=w1, dst=lambda z, y, x, c: g1.at[x * 2 + c, pl.ds(pl.multiple_of((z * 2 + y) * 128, 128), 128), :], half=hrows(64)),
        dict(src=w2, dst=lambda z, y, x, c: g2.at[x * 2 + c, :, pl.ds(pl.multiple_of((z * 2 + y) * 128, 128), 128)], half=hrows(512)),
    ]

def schedule(n, lag=5):
    one = [("own", 0), ("avail", 1), ("near", 0), ("avail", 2), ("near", 1), ("opp", 0), ("avail", 3), ("near", 2), ("opp", 1), ("near", 3), ("opp", 2), ("opp", 3)]
    ev = []
    for g in range(n):
        for i, s in enumerate(one):
            ev.append((g * 12 + i - (lag if i < 12 - lag else 0) * 0 - g * lag, g, i, s))
    ev.sort(key=lambda t: (t[0], t[1]))
    return [(g, s) for _, g, _, s in ev]

def gather_kernel(lag, qkv, out, w1, w2, gq, go, g1, g2, *sems):
    G = Gather(make_groups(qkv, out, w1, w2, gq, go, g1, g2), sems)
    G.barrier()
    for g, (kind, e) in schedule(4, lag):
        getattr(G, kind)(*((g,) if kind == "own" else (g, e)))
    for g in range(4):
        for e in range(4): G.partner(g, e)
        G.local(g); G.sent(g)

def gather_all(qkv, out, w1, w2, lag=5):
    any_ = pl.BlockSpec(memory_space=pl.ANY); vm = pl.BlockSpec(memory_space=pltpu.VMEM)
    bf = jnp.bfloat16
    S = jax.ShapeDtypeStruct
    return pl.pallas_call(
        functools.partial(gather_kernel, lag),
        out_shape=(S((3072, 1024), bf), S((1024, 1024), bf), S((4, 1024, 1024), bf), S((4, 1024, 1024), bf)),
        in_specs=[vm] * 4, out_specs=(any_,) * 4,
        scratch_shapes=sem_shapes(4),
        compiler_params=pltpu.CompilerParams(collective_id=1, has_side_effects=True),
        name="gather_weights",
    )(qkv, out, w1, w2)
HEADS = 16
HEAD = 64
BF = jnp.bfloat16
F32 = jnp.float32
NN = (((1,), (0,)), ((), ()))
NT = (((1,), (1,)), ((), ()))
TAIL = (0.11962929488154013, 0.12075401780706921, 0.09991309952872984, 0.1285629430504706,
        -0.053686168541539216, 0.20635628544846257, -0.15720471604044917, 0.03567517103968566)


def dot(a, b, dims=NN):
    return lax.dot_general(a, b, dims, preferred_element_type=F32)


def gelu_and_slope(v):
    a = jnp.abs(v)
    t = 1.0 / (1.0 + 0.3 * a)
    e = jnp.exp(-0.5 * v * v)
    r = jnp.full_like(v, TAIL[7])
    for c in TAIL[6::-1]:
        r = r * t + c
    tail = r * t * e
    cdf = jnp.where(v < 0, tail, 1.0 - tail)
    return v * cdf, cdf + v * (e * 0.3989422804014327)


def norm_rows(r):
    mean = jnp.mean(r, axis=-1, keepdims=True)
    cent = r - mean
    inv = lax.rsqrt(jnp.mean(cent * cent, axis=-1, keepdims=True) + 1e-12)
    return cent * inv, inv


def norm_back(u, n, inv, gain):
    s = u * gain
    return inv * (s - jnp.mean(s, axis=-1, keepdims=True) - n * jnp.mean(s * n, axis=-1, keepdims=True))


def colsum(a):
    return jnp.sum(a, axis=0, keepdims=True)


def head_lanes(rows):
    return lax.broadcasted_iota(jnp.int32, (rows, 2 * HEAD), 1) < HEAD


def keep_head(a, h, lanes):
    z = jnp.zeros_like(a)
    return jnp.where(lanes, a, z) if h == 0 else jnp.where(lanes, z, a)


def attend(q, k, v, length):
    seq = q.shape[0]
    lanes = head_lanes(seq)
    ks = k * jnp.asarray(0.125, BF)
    vt = v.T
    valid = lax.broadcasted_iota(jnp.int32, (seq, 1), 0) < length
    bias = jnp.where(valid, 0.0, -1e9)
    outs, totals = [], []
    for h in range(2):
        s = dot(keep_head(ks, h, lanes), q, NT) + bias
        top = jnp.max(s, axis=0, keepdims=True)
        p = jnp.exp(s - top)
        total = jnp.sum(p, axis=0, keepdims=True)
        outs.append(dot(vt[h * HEAD:(h + 1) * HEAD, :], p.astype(BF)) * (1.0 / total))
        totals.append(top + jnp.log(total))
    return jnp.concatenate(outs, axis=0).T.astype(BF), totals


def attend_back(q, k, v, dc, length, totals):
    seq = q.shape[0]
    lanes = head_lanes(seq)
    ks = k * jnp.asarray(0.125, BF)
    kt = ks.T
    valid = lax.broadcasted_iota(jnp.int32, (seq, 1), 0) < length
    bias = jnp.where(valid, 0.0, -1e9)
    dq, dk, dv = [], [], []
    for h in range(2):
        s = dot(keep_head(ks, h, lanes), q, NT) + bias
        p = jnp.exp(s - totals[h])
        dp = dot(keep_head(v, h, lanes), dc, NT)
        row = jnp.sum(p * dp, axis=0, keepdims=True)
        ds = (p * (dp - row)).astype(BF)
        dv.append(dot(p.astype(BF), dc))
        dk.append(dot(ds, q))
        dq.append(dot(kt[h * HEAD:(h + 1) * HEAD, :], ds))
    dq = jnp.concatenate(dq, axis=0).T
    return dq.astype(BF), (jnp.where(lanes, dk[0], dk[1]) * 0.125).astype(BF), jnp.where(lanes, dv[0], dv[1]).astype(BF)


def lane(i, n):
    return pl.ds(pl.multiple_of(i * n, n), n)


def embed(tok, seg, table):
    t = table.astype(F32)
    return tok.astype(F32) + jnp.where(seg == 1, t[1:2, :], t[0:1, :])


def project_qkv(tok, seg, table, bias, wq, qkv, step=256, pump=None):
    for m in range(3):
        def body(i, _):
            r = lane(i, step)
            x = embed(tok[r, :], seg[r, :], table[...]).astype(BF)
            y = dot(x, wq[m * 1024:(m + 1) * 1024, :])
            if m != 1:
                y = y + bias[m // 2:m // 2 + 1, :].astype(F32)
            qkv[m, r, :] = y.astype(BF)
            return 0
        lax.fori_loop(0, tok.shape[0] // step, body, 0)
        if pump: pump()


def attention(qkv, lengths, ctx, totals, seq, s, first, count):
    def body(i, _):
        rows = pl.ds(s * seq, seq)
        cols = lane(i, 128)
        c, t = attend(qkv[0, rows, cols], qkv[1, rows, cols], qkv[2, rows, cols], lengths[s])
        ctx[rows, cols] = c
        for h in range(2):
            totals[pl.ds(s * HEADS + i * 2 + h, 1), :] = t[h]
        return 0
    lax.fori_loop(first, first + count, body, 0)


def middle_rows(r, tok, seg, table, ctx, wo, bias, normed, inv):
    res = embed(tok[r, :], seg[r, :], table[...]) + (dot(ctx[r, :], wo[...]) + bias[2:3, :].astype(F32))
    n, i = norm_rows(res)
    normed[r, :] = n
    inv[r, :] = i


def expand_rows(r, t, w1t, normed, gain, shift, bias1, hidden, slope):
    mid = normed[r, :] * gain[0:1, :].astype(F32) + shift[0:1, :].astype(F32)
    cols = lane(t, 1024)
    v = dot(mid.astype(BF), w1t) + bias1[:, cols].astype(F32)
    h, g = gelu_and_slope(v)
    hidden[r, cols] = h.astype(BF)
    slope[r, cols] = g.astype(BF)


def mlp_kernel(hid, slp, nrm, inv1, cot, w1, w2, wo, gain, shift, bias2,
               out, dfirst, dctx, g_bo, g_b1, g_b2, g_gain, g_shift):
    @pl.when(pl.program_id(0) == 0)
    def _():
        for ref in (g_bo, g_b1, g_b2, g_gain, g_shift):
            ref[...] = jnp.zeros_like(ref)
    ga, sh = gain[...].astype(F32), shift[...].astype(F32)
    n1 = nrm[...]
    res = n1 * ga[0:1] + sh[0:1] + bias2[...].astype(F32)
    for t in range(4):
        res = res + dot(hid[:, t * 1024:(t + 1) * 1024], w2[t])
    n2, inv2 = norm_rows(res)
    out[...] = (n2 * ga[1:2] + sh[1:2]).astype(BF)
    u = cot[...].astype(F32)
    g_gain[1:2, :] += colsum(u * n2)
    g_shift[1:2, :] += colsum(u)
    d2 = norm_back(u, n2, inv2, ga[1:2])
    db = d2.astype(BF)
    g_b2[...] += colsum(db.astype(F32))
    dmid = d2
    for t in range(4):
        c = slice(t * 1024, (t + 1) * 1024)
        dpre = (dot(db, w2[t], NT) * slp[:, c].astype(F32)).astype(BF)
        g_b1[:, c] += colsum(dpre.astype(F32))
        dmid = dmid + dot(dpre, w1[t], NT)
    g_gain[0:1, :] += colsum(dmid * n1)
    g_shift[0:1, :] += colsum(dmid)
    d1 = norm_back(dmid, n1, inv1[...], ga[0:1])
    dfirst[...] = d1
    da = d1.astype(BF)
    g_bo[...] += colsum(da.astype(F32))
    dctx[...] = dot(da, wo[...], NT).astype(BF)


def mlp_call(hid, slp, nrm, inv1, cot, w1, w2, wo, gain, shift, bias2, rows=256):
    tok, d = cot.shape
    ff = hid.shape[1]
    S = jax.ShapeDtypeStruct
    row = lambda n: pl.BlockSpec((rows, n), lambda i: (i, 0))
    one = lambda a: pl.BlockSpec(a.shape, lambda i: (0,) * a.ndim, pipeline_mode=pl.Buffered(1))
    acc = lambda a, b: pl.BlockSpec((a, b), lambda i: (0, 0))
    return pl.pallas_call(
        mlp_kernel,
        grid=(tok // rows,),
        in_specs=[row(ff), row(ff), row(d), row(1), row(d), one(w1), one(w2), one(wo), one(gain), one(shift), one(bias2)],
        out_specs=[row(d), row(d), row(d), acc(1, d), acc(1, ff), acc(1, d), acc(2, d), acc(2, d)],
        out_shape=[S((tok, d), BF), S((tok, d), F32), S((tok, d), BF), S((1, d), F32), S((1, ff), F32), S((1, d), F32), S((2, d), F32), S((2, d), F32)],
        compiler_params=pltpu.CompilerParams(vmem_limit_bytes=62 * 1024 * 1024, dimension_semantics=("arbitrary",)),
        name="mlp",
    )(hid, slp, nrm, inv1, cot, w1, w2, wo, gain, shift, bias2)


def back_kernel(lengths, q, k, v, dc, tot, dfirst, wq, gin, g_q, g_v, grads):
    s, i = pl.program_id(0), pl.program_id(1)
    @pl.when((s == 0) & (i == 0))
    def _():
        g_q[...] = jnp.zeros_like(g_q)
        g_v[...] = jnp.zeros_like(g_v)
    t = [tot[pl.ds(s * HEADS + i * 2 + h, 1), :] for h in range(2)]
    dq, dk, dv = attend_back(q[0], k[0], v[0], dc[...], lengths[s], t)
    cols = lane(i, 128)
    g_q[:, cols] += colsum(dq.astype(F32))
    g_v[:, cols] += colsum(dv.astype(F32))
    for m, a in enumerate((dq, dk, dv)):
        grads[m, :, cols] = a
    @pl.when(i == pl.num_programs(1) - 1)
    def _():
        def body(j, _):
            r = lane(j, 256)
            acc = dfirst[r, :]
            for m in range(3):
                acc = acc + dot(grads[m, r, :], wq[m * 1024:(m + 1) * 1024, :], NT)
            gin[r, :] = acc.astype(BF)
            return 0
        lax.fori_loop(0, gin.shape[0] // 256, body, 0)


def back_call(lengths, qkv, dctx, totals, dfirst, wq, seq):
    tok, d = dctx.shape
    S = jax.ShapeDtypeStruct
    head = lambda m: pl.BlockSpec((1, seq, 128), lambda s, i, ln: (m, s, i))
    return pl.pallas_call(
        back_kernel,
        grid_spec=pltpu.PrefetchScalarGridSpec(
            num_scalar_prefetch=1,
            grid=(tok // seq, d // 128),
            in_specs=[head(0), head(1), head(2), pl.BlockSpec((seq, 128), lambda s, i, ln: (s, i)),
                      pl.BlockSpec(totals.shape, lambda s, i, ln: (0, 0), pipeline_mode=pl.Buffered(1)),
                      pl.BlockSpec((seq, d), lambda s, i, ln: (s, 0)),
                      pl.BlockSpec(wq.shape, lambda s, i, ln: (0, 0), pipeline_mode=pl.Buffered(1))],
            out_specs=[pl.BlockSpec((seq, d), lambda s, i, ln: (s, 0)), pl.BlockSpec((1, d), lambda s, i, ln: (0, 0)), pl.BlockSpec((1, d), lambda s, i, ln: (0, 0))],
            scratch_shapes=[pltpu.VMEM((3, seq, d), BF)],
        ),
        out_shape=[S((tok, d), BF), S((1, d), F32), S((1, d), F32)],
        compiler_params=pltpu.CompilerParams(vmem_limit_bytes=62 * 1024 * 1024, dimension_semantics=("arbitrary", "arbitrary")),
        name="attention_back",
    )(lengths, qkv, qkv, qkv, dctx, totals, dfirst, wq)
def front_kernel(seq, lengths, tok, seg, table, wq, wo, w1, bias, bias1, gain, shift, qkv, totals, normed, inv, hidden, slope, ctx):
    project_qkv(tok, seg, table, bias, wq, qkv)
    n = tok.shape[0]
    for s in range(n // seq):
        attention(qkv, lengths, ctx, totals, seq, s, 0, qkv.shape[2] // 128)
    def mid(i, _):
        middle_rows(lane(i, 256), tok, seg, table, ctx, wo, bias, normed, inv)
        return 0
    lax.fori_loop(0, n // 256, mid, 0)
    def exp(j, _):
        t, i = j // (n // 256), j % (n // 256)
        expand_rows(lane(i, 256), t, w1[t], normed, gain, shift, bias1, hidden, slope)
        return 0
    lax.fori_loop(0, 4 * (n // 256), exp, 0)


def front_call(lengths, tok, seg, table, wq, wo, w1, bias, bias1, gain, shift, seq):
    n, d = tok.shape
    ff = bias1.shape[1]
    S = jax.ShapeDtypeStruct
    vm = pl.BlockSpec(memory_space=pltpu.VMEM)
    return pl.pallas_call(
        functools.partial(front_kernel, seq),
        in_specs=[pl.BlockSpec(memory_space=pltpu.SMEM)] + [vm] * 10,
        out_specs=[vm] * 6,
        out_shape=[S((3, n, d), BF), S((n // seq * HEADS, seq), F32), S((n, d), F32), S((n, 1), F32), S((n, ff), BF), S((n, ff), BF)],
        scratch_shapes=[pltpu.VMEM((n, d), BF)],
        compiler_params=pltpu.CompilerParams(vmem_limit_bytes=64 * 1024 * 1024 - 65536),
        name="front",
    )(lengths, tok, seg, table, wq, wo, w1, bias, bias1, gain, shift)


def per_device(tokens, segments, lengths, type_table, attn_weight, out_weight, ffn_in_weight, ffn_out_weight, attn_bias,
               ffn_bias_in, ffn_bias_out, norm_gain, norm_shift, cotangent):
    n, d = tokens.shape
    seq = segments.shape[1]
    if ffn_in_weight.shape == (128, 1024) and lax.axis_size("dp") == 8 and lax.axis_size("tensor") == 4:
        wq, wo, w1, w2 = gather_all(attn_weight.reshape(-1, d), out_weight.reshape(-1, d), ffn_in_weight, ffn_out_weight, 12)
    else:
        wq = lax.all_gather(attn_weight, ("dp", "tensor"), axis=0, tiled=True).reshape(-1, d)
        wo = lax.all_gather(out_weight, ("dp", "tensor"), axis=0, tiled=True).reshape(-1, d)
        w1 = lax.all_gather(lax.all_gather(ffn_in_weight, "dp", axis=0, tiled=True), "tensor", axis=1, tiled=True)
        w1 = w1.reshape(d, 4, -1).transpose(1, 0, 2)
        w2 = lax.all_gather(lax.all_gather(ffn_out_weight, "dp", axis=1, tiled=True), "tensor", axis=0, tiled=True).reshape(4, -1, d)
    qkv, totals, normed, inv, hidden, slope = front_call(
        lengths, tokens, segments.reshape(-1, 1), type_table, wq, wo, w1, attn_bias, ffn_bias_in[None], norm_gain, norm_shift, seq)
    output, dfirst, dctx, g_bo, g_b1, g_b2, g_gain, g_shift = mlp_call(
        hidden, slope, normed, inv, cotangent, w1, w2, wo, norm_gain, norm_shift, ffn_bias_out[None])
    grad_input, g_q, g_v = back_call(lengths, qkv, dctx, totals, dfirst, wq, seq)
    g_attn = jnp.concatenate([g_q, g_v, g_bo], axis=0)
    sums = lax.psum((g_attn, g_b1[0], g_b2[0], g_gain, g_shift), ("dp", "tensor"))
    return (output, grad_input) + tuple(sums)


def solution(mesh):
    rows = P(("dp", "tensor"), None)
    flat = P(("dp", "tensor"))
    in_specs = (rows, rows, flat, P(), flat, flat, P("dp", "tensor"), P("tensor", "dp"), P(), P(), P(), P(), P(), rows)
    return jax.shard_map(per_device, mesh=mesh, in_specs=in_specs, out_specs=(rows, rows, P(), P(), P(), P(), P()), check_vma=False)
```

```python
import functools, math
import jax, jax.numpy as jnp
from jax import lax
from jax.sharding import PartitionSpec as P
from jax.experimental import pallas as pl
from jax.experimental.pallas import tpu as pltpu
MESH = pl.DeviceIdType.MESH

class Gather:
    def __init__(self, groups, sems):
        dp = lax.axis_index("dp"); tn = lax.axis_index("tensor")
        self.z, self.y = dp // 2, dp % 2
        self.x, self.c = tn // 2, tn % 2
        self.inner = (self.z + 1) // 2 % 2
        self.groups = groups
        self.zs, self.zr, self.xs, self.xr, self.ys, self.yr, self.hs, self.hr, self.ds, self.dr, self.loc = sems
        self.todo = []

    def zz(self, e):
        z = self.z
        return [z, z + 1 - 2 * (z % 2), 2 - z // 2, 3 * (1 - z // 2)][e]

    def dev(self, z, y, x, c):
        return (z * 2 + y, x * 2 + c)

    def copy(self, src, dst, ss, rs, dev):
        return pltpu.make_async_remote_copy(src_ref=src, dst_ref=dst, send_sem=ss, recv_sem=rs, device_id=dev, device_id_type=MESH)

    def barrier(self):
        b = pltpu.get_barrier_semaphore()
        z, y, x, c = self.z, self.y, self.x, self.c
        for d in ((z, y, x, 1 - c), (z, y, 1 - x, c), (z, 1 - y, x, c), (self.zz(1), y, x, c)):
            pl.semaphore_signal(b, inc=1, device_id=self.dev(*d), device_id_type=MESH)
        @pl.when(self.inner == 1)
        def _():
            pl.semaphore_signal(b, inc=1, device_id=self.dev(3 - z, y, x, c), device_id_type=MESH)
            pl.semaphore_wait(b, 5)
        @pl.when(self.inner == 0)
        def _():
            pl.semaphore_wait(b, 4)

    def zcopy(self, g, e, k, pair):
        z, y, x, c = self.z, self.y, self.x, self.c
        G = self.groups[g]; zp = self.zz(e)
        view = G["dst"](zp, y, x, c)
        src = G["src"] if e == 0 else view
        to = self.zz(1) if pair else 3 - z
        return self.copy(src, view, self.zs.at[g, k], self.zr.at[g, zp], self.dev(to, y, x, c))

    def zrecv(self, g, e):
        z, y, x, c = self.z, self.y, self.x, self.c
        zp = self.zz(e); view = self.groups[g]["dst"](zp, y, x, c)
        return self.copy(view, view, self.zs.at[g, 0], self.zr.at[g, zp], self.dev(self.zz(1), y, x, c))

    def ncopy(self, g, e, ax):
        z, y, x, c = self.z, self.y, self.x, self.c
        G = self.groups[g]; zp = self.zz(e)
        view = G["dst"](zp, y, x, c)
        src = G["src"] if e == 0 else view
        S, R = (self.xs, self.xr) if ax == "x" else (self.ys, self.yr)
        to = self.dev(z, y, 1 - x, c) if ax == "x" else self.dev(z, 1 - y, x, c)
        return self.copy(src, view, S.at[g, e], R.at[g, e], to)

    def nrecv(self, g, e, ax):
        z, y, x, c = self.z, self.y, self.x, self.c
        view = self.groups[g]["dst"](self.zz(e), y, 1 - x, c) if ax == "x" else self.groups[g]["dst"](self.zz(e), 1 - y, x, c)
        S, R = (self.xs, self.xr) if ax == "x" else (self.ys, self.yr)
        return self.copy(view, view, S.at[g, e], R.at[g, e], self.dev(z, y, x, 1 - c))

    def hcopy(self, g, e, h):
        z, y, x, c = self.z, self.y, self.x, self.c
        G = self.groups[g]; zp = self.zz(e)
        full = G["dst"](zp, 1 - y, x, c) if h == 0 else G["dst"](zp, y, 1 - x, c)
        v = G["half"](full, h)
        to = self.dev(z, y, 1 - x, c) if h == 0 else self.dev(z, 1 - y, x, c)
        return self.copy(v, v, self.hs.at[g, e, h], self.hr.at[g, e, h], to)

    def hrecv(self, g, e, h):
        z, y, x, c = self.z, self.y, self.x, self.c
        G = self.groups[g]
        v = G["half"](G["dst"](self.zz(e), 1 - y, 1 - x, c), h)
        return self.copy(v, v, self.hs.at[g, e, h], self.hr.at[g, e, h], self.dev(z, y, x, 1 - c))

    def dcopy(self, g, e, k, recv=False):
        z, y, x, c = self.z, self.y, self.x, self.c
        G = self.groups[g]; zp = self.zz(e)
        cc = 1 - c if recv else c
        if k == 0: v = G["dst"](zp, y, x, cc)
        elif k == 1: v = G["dst"](zp, y, 1 - x, cc)
        elif k == 2: v = G["dst"](zp, 1 - y, x, cc)
        else: v = G["half"](G["dst"](zp, 1 - y, 1 - x, cc), k - 3)
        src = G["src"] if (e == 0 and k == 0 and not recv) else v
        return self.copy(src, v, self.ds.at[g, e, k], self.dr.at[g, e, k], self.dev(z, y, x, 1 - c))

    def own(self, g):
        G = self.groups[g]
        self.zcopy(g, 0, 0, True).start()
        @pl.when(self.inner == 1)
        def _(): self.zcopy(g, 0, 1, False).start()
        self.ncopy(g, 0, "x").start(); self.ncopy(g, 0, "y").start()
        pltpu.make_async_copy(G["src"], G["dst"](self.z, self.y, self.x, self.c), self.loc.at[g]).start()
        self.dcopy(g, 0, 0).start()

    def avail(self, g, e):
        self.zrecv(g, e).wait_recv()
        @pl.when(self.inner == 1)
        def _(): self.zcopy(g, e, e + 1, e != 1).start()
        self.ncopy(g, e, "x").start(); self.ncopy(g, e, "y").start()
        self.dcopy(g, e, 0).start()

    def near(self, g, e):
        self.nrecv(g, e, "x").wait_recv()
        self.hcopy(g, e, 1).start()
        self.dcopy(g, e, 1).start()
        self.nrecv(g, e, "y").wait_recv()
        self.hcopy(g, e, 0).start()
        self.dcopy(g, e, 2).start()

    def opp(self, g, e):
        for h in (0, 1):
            self.hrecv(g, e, h).wait_recv()
            self.dcopy(g, e, 3 + h).start()

    def partner(self, g, e):
        for k in range(5): self.dcopy(g, e, k, recv=True).wait_recv()

    def local(self, g):
        G = self.groups[g]
        pltpu.make_async_copy(G["src"], G["dst"](self.z, self.y, self.x, self.c), self.loc.at[g]).wait()

    def sent(self, g):
        self.zcopy(g, 0, 0, True).wait_send()
        @pl.when(self.inner == 1)
        def _():
            self.zcopy(g, 0, 1, False).wait_send()
            for e in (1, 2, 3): self.zcopy(g, e, e + 1, e != 1).wait_send()
        for e in range(4):
            self.ncopy(g, e, "x").wait_send(); self.ncopy(g, e, "y").wait_send()
            for h in (0, 1): self.hcopy(g, e, h).wait_send()
            for k in range(5): self.dcopy(g, e, k).wait_send()

    def finish(self, g):
        for e in range(4):
            self.partner(g, e)
        self.local(g)

def sem_shapes(n):
    D = pltpu.SemaphoreType.DMA
    return [D((n, 5)), D((n, 4)), D((n, 4)), D((n, 4)), D((n, 4)), D((n, 4)), D((n, 4, 2)), D((n, 4, 2)), D((n, 4, 5)), D((n, 4, 5)), D((n,))]

def make_groups(qkv, out, w1, w2, gq, go, g1, g2):
    lin = lambda z, y, x, c: ((z * 2 + y) * 2 + x) * 2 + c
    def rows(ref, n):
        return lambda z, y, x, c: ref.at[pl.ds(pl.multiple_of(lin(z, y, x, c) * n, n), n), :]
    def hrows(n):
        return lambda v, h: v.at[pl.ds(h * n, n), :]
    return [
        dict(src=qkv, dst=rows(gq, 96), half=hrows(48)),
        dict(src=out, dst=rows(go, 32), half=hrows(16)),
        dict(src=w1, dst=lambda z, y, x, c: g1.at[x * 2 + c, pl.ds(pl.multiple_of((z * 2 + y) * 128, 128), 128), :], half=hrows(64)),
        dict(src=w2, dst=lambda z, y, x, c: g2.at[x * 2 + c, :, pl.ds(pl.multiple_of((z * 2 + y) * 128, 128), 128)], half=hrows(512)),
    ]

ORDER = (("own", 0), ("avail", 1), ("near", 0), ("avail", 2), ("near", 1), ("opp", 0), ("avail", 3), ("near", 2), ("opp", 1), ("near", 3), ("opp", 2), ("opp", 3))


def schedule(n, lag):
    ev = sorted(((g * (len(ORDER) - lag) + i, g, s) for g in range(n) for i, s in enumerate(ORDER)), key=lambda t: t[:2])
    return [(g, s) for _, g, s in ev]
HEADS = 16
HEAD = 64
BF = jnp.bfloat16
F32 = jnp.float32
NN = (((1,), (0,)), ((), ()))
NT = (((1,), (1,)), ((), ()))
TAIL = (0.11962929488154013, 0.12075401780706921, 0.09991309952872984, 0.1285629430504706,
        -0.053686168541539216, 0.20635628544846257, -0.15720471604044917, 0.03567517103968566)


def dot(a, b, dims=NN):
    return lax.dot_general(a, b, dims, preferred_element_type=F32)


def gelu_and_slope(v):
    a = jnp.abs(v)
    t = 1.0 / (1.0 + 0.3 * a)
    e = jnp.exp(-0.5 * v * v)
    r = jnp.full_like(v, TAIL[7])
    for c in TAIL[6::-1]:
        r = r * t + c
    tail = r * t * e
    cdf = jnp.where(v < 0, tail, 1.0 - tail)
    return v * cdf, cdf + v * (e * 0.3989422804014327)


def norm_rows(r):
    mean = jnp.mean(r, axis=-1, keepdims=True)
    cent = r - mean
    inv = lax.rsqrt(jnp.mean(cent * cent, axis=-1, keepdims=True) + 1e-12)
    return cent * inv, inv


def norm_back(u, n, inv, gain):
    s = u * gain
    return inv * (s - jnp.mean(s, axis=-1, keepdims=True) - n * jnp.mean(s * n, axis=-1, keepdims=True))


def colsum(a):
    return jnp.sum(a, axis=0, keepdims=True)


def head_lanes(rows):
    return lax.broadcasted_iota(jnp.int32, (rows, 2 * HEAD), 1) < HEAD


def keep_head(a, h, lanes):
    z = jnp.zeros_like(a)
    return jnp.where(lanes, a, z) if h == 0 else jnp.where(lanes, z, a)


def attend(q, k, v, length):
    seq = q.shape[0]
    lanes = head_lanes(seq)
    ks = k * jnp.asarray(0.125, BF)
    vt = v.T
    valid = lax.broadcasted_iota(jnp.int32, (seq, 1), 0) < length
    bias = jnp.where(valid, 0.0, -1e9)
    outs, totals = [], []
    for h in range(2):
        s = dot(keep_head(ks, h, lanes), q, NT) + bias
        top = jnp.max(s, axis=0, keepdims=True)
        p = jnp.exp(s - top)
        total = jnp.sum(p, axis=0, keepdims=True)
        outs.append(dot(vt[h * HEAD:(h + 1) * HEAD, :], p.astype(BF)) * (1.0 / total))
        totals.append(top + jnp.log(total))
    return jnp.concatenate(outs, axis=0).T.astype(BF), totals


def attend_back(q, k, v, dc, length, totals):
    seq = q.shape[0]
    lanes = head_lanes(seq)
    ks = k * jnp.asarray(0.125, BF)
    kt = ks.T
    valid = lax.broadcasted_iota(jnp.int32, (seq, 1), 0) < length
    bias = jnp.where(valid, 0.0, -1e9)
    dq, dk, dv = [], [], []
    for h in range(2):
        s = dot(keep_head(ks, h, lanes), q, NT) + bias
        p = jnp.exp(s - totals[h])
        dp = dot(keep_head(v, h, lanes), dc, NT)
        row = jnp.sum(p * dp, axis=0, keepdims=True)
        ds = (p * (dp - row)).astype(BF)
        dv.append(dot(p.astype(BF), dc))
        dk.append(dot(ds, q))
        dq.append(dot(kt[h * HEAD:(h + 1) * HEAD, :], ds))
    dq = jnp.concatenate(dq, axis=0).T
    return dq.astype(BF), (jnp.where(lanes, dk[0], dk[1]) * 0.125).astype(BF), jnp.where(lanes, dv[0], dv[1]).astype(BF)


def lane(i, n):
    return pl.ds(pl.multiple_of(i * n, n), n)


def embed(tok, seg, table):
    t = table.astype(F32)
    return tok.astype(F32) + jnp.where(seg == 1, t[1:2, :], t[0:1, :])


def middle_rows(r, tok, seg, table, ctx, wo, bias, normed, inv):
    res = embed(tok[r, :], seg[r, :], table[...]) + (dot(ctx[r, :], wo[...]) + bias[2:3, :].astype(F32))
    n, i = norm_rows(res)
    normed[r, :] = n
    inv[r, :] = i


def expand_rows(r, t, w1t, normed, gain, shift, bias1, hidden, slope):
    mid = normed[r, :] * gain[0:1, :].astype(F32) + shift[0:1, :].astype(F32)
    cols = lane(t, 1024)
    v = dot(mid.astype(BF), w1t) + bias1[:, cols].astype(F32)
    h, g = gelu_and_slope(v)
    hidden[r, cols] = h.astype(BF)
    slope[r, cols] = g.astype(BF)


def mlp_kernel(hid, slp, nrm, inv1, cot, w1, w2, wo, gain, shift, bias2,
               out, dfirst, dctx, g_bo, g_b1, g_b2, g_gain, g_shift):
    @pl.when(pl.program_id(0) == 0)
    def _():
        for ref in (g_bo, g_b1, g_b2, g_gain, g_shift):
            ref[...] = jnp.zeros_like(ref)
    ga, sh = gain[...].astype(F32), shift[...].astype(F32)
    n1 = nrm[...]
    res = n1 * ga[0:1] + sh[0:1] + bias2[...].astype(F32)
    for t in range(4):
        res = res + dot(hid[:, t * 1024:(t + 1) * 1024], w2[t])
    n2, inv2 = norm_rows(res)
    out[...] = (n2 * ga[1:2] + sh[1:2]).astype(BF)
    u = cot[...].astype(F32)
    g_gain[1:2, :] += colsum(u * n2)
    g_shift[1:2, :] += colsum(u)
    d2 = norm_back(u, n2, inv2, ga[1:2])
    db = d2.astype(BF)
    g_b2[...] += colsum(db.astype(F32))
    dmid = d2
    for t in range(4):
        c = slice(t * 1024, (t + 1) * 1024)
        dpre = (dot(db, w2[t], NT) * slp[:, c].astype(F32)).astype(BF)
        g_b1[:, c] += colsum(dpre.astype(F32))
        dmid = dmid + dot(dpre, w1[t], NT)
    g_gain[0:1, :] += colsum(dmid * n1)
    g_shift[0:1, :] += colsum(dmid)
    d1 = norm_back(dmid, n1, inv1[...], ga[0:1])
    dfirst[...] = d1
    da = d1.astype(BF)
    g_bo[...] += colsum(da.astype(F32))
    dctx[...] = dot(da, wo[...], NT).astype(BF)


def mlp_call(hid, slp, nrm, inv1, cot, w1, w2, wo, gain, shift, bias2, rows=256):
    tok, d = cot.shape
    ff = hid.shape[1]
    S = jax.ShapeDtypeStruct
    row = lambda n: pl.BlockSpec((rows, n), lambda i: (i, 0))
    one = lambda a: pl.BlockSpec(a.shape, lambda i: (0,) * a.ndim, pipeline_mode=pl.Buffered(1))
    acc = lambda a, b: pl.BlockSpec((a, b), lambda i: (0, 0))
    return pl.pallas_call(
        mlp_kernel,
        grid=(tok // rows,),
        in_specs=[row(ff), row(ff), row(d), row(1), row(d), one(w1), one(w2), one(wo), one(gain), one(shift), one(bias2)],
        out_specs=[row(d), row(d), row(d), acc(1, d), acc(1, ff), acc(1, d), acc(2, d), acc(2, d)],
        out_shape=[S((tok, d), BF), S((tok, d), F32), S((tok, d), BF), S((1, d), F32), S((1, ff), F32), S((1, d), F32), S((2, d), F32), S((2, d), F32)],
        compiler_params=pltpu.CompilerParams(vmem_limit_bytes=62 * 1024 * 1024, dimension_semantics=("arbitrary",)),
        name="mlp",
    )(hid, slp, nrm, inv1, cot, w1, w2, wo, gain, shift, bias2)


def back_kernel(lengths, q, k, v, dc, tot, dfirst, wq, gin, g_q, g_v, grads):
    s, i = pl.program_id(0), pl.program_id(1)
    @pl.when((s == 0) & (i == 0))
    def _():
        g_q[...] = jnp.zeros_like(g_q)
        g_v[...] = jnp.zeros_like(g_v)
    t = [tot[pl.ds(s * HEADS + i * 2 + h, 1), :] for h in range(2)]
    dq, dk, dv = attend_back(q[0], k[0], v[0], dc[...], lengths[s], t)
    cols = lane(i, 128)
    g_q[:, cols] += colsum(dq.astype(F32))
    g_v[:, cols] += colsum(dv.astype(F32))
    for m, a in enumerate((dq, dk, dv)):
        grads[m, :, cols] = a
    @pl.when(i == pl.num_programs(1) - 1)
    def _():
        def body(j, _):
            r = lane(j, 256)
            acc = dfirst[r, :]
            for m in range(3):
                acc = acc + dot(grads[m, r, :], wq[m * 1024:(m + 1) * 1024, :], NT)
            gin[r, :] = acc.astype(BF)
            return 0
        lax.fori_loop(0, gin.shape[0] // 256, body, 0)


def back_call(lengths, qkv, dctx, totals, dfirst, wq, seq):
    tok, d = dctx.shape
    S = jax.ShapeDtypeStruct
    head = lambda m: pl.BlockSpec((1, seq, 128), lambda s, i, ln: (m, s, i))
    return pl.pallas_call(
        back_kernel,
        grid_spec=pltpu.PrefetchScalarGridSpec(
            num_scalar_prefetch=1,
            grid=(tok // seq, d // 128),
            in_specs=[head(0), head(1), head(2), pl.BlockSpec((seq, 128), lambda s, i, ln: (s, i)),
                      pl.BlockSpec(totals.shape, lambda s, i, ln: (0, 0), pipeline_mode=pl.Buffered(1)),
                      pl.BlockSpec((seq, d), lambda s, i, ln: (s, 0)),
                      pl.BlockSpec(wq.shape, lambda s, i, ln: (0, 0), pipeline_mode=pl.Buffered(1))],
            out_specs=[pl.BlockSpec((seq, d), lambda s, i, ln: (s, 0)), pl.BlockSpec((1, d), lambda s, i, ln: (0, 0)), pl.BlockSpec((1, d), lambda s, i, ln: (0, 0))],
            scratch_shapes=[pltpu.VMEM((3, seq, d), BF)],
        ),
        out_shape=[S((tok, d), BF), S((1, d), F32), S((1, d), F32)],
        compiler_params=pltpu.CompilerParams(vmem_limit_bytes=62 * 1024 * 1024, dimension_semantics=("arbitrary", "arbitrary")),
        name="attention_back",
    )(lengths, qkv, qkv, qkv, dctx, totals, dfirst, wq)
LAG = 4


class Pump:
    def __init__(self, G):
        self.G = G
        self.ev = schedule(4, LAG) if G else []

    def step(self):
        g, (kind, e) = self.ev.pop(0)
        getattr(self.G, kind)(*((g,) if kind == "own" else (g, e)))

    def until(self, g):
        if self.G:
            while any(v[0] == g for v in self.ev):
                self.step()
            self.G.finish(g)

    def loop(self, count, body, every=1):
        take = self.ev[:count // every]
        del self.ev[:count // every]

        def unit(i, _):
            body(i)
            for k, (g, (kind, e)) in enumerate(take):
                @pl.when(i == k * every + every - 1)
                def _():
                    getattr(self.G, kind)(*((g,) if kind == "own" else (g, e)))
            return 0
        lax.fori_loop(0, count, unit, 0)


def front_kernel(seq, gathers, lengths, tok, seg, table, bias, bias1, gain, shift, *refs):
    if gathers:
        shards, refs = refs[:4], refs[4:]
        hq, ho, h1, h2 = refs[:4]
    else:
        hq, ho, h1, h2 = refs[:4]
    qkv_o, totals, normed_o, inv, hidden_o, slope_o = refs[4:10]
    qkv, ctx, normed, hidden, slope, wq, wo, w1, wsem, osem = refs[10:20]
    n = tok.shape[0]
    steps = n // 256
    G = None
    if gathers:
        G = Gather(make_groups(*shards, hq, ho, h1, h2), refs[20:])
        G.barrier()
    pump = Pump(G)
    outs = []

    def load(src, dst, k):
        c = pltpu.make_async_copy(src, dst, wsem.at[k])
        c.start()
        return c

    def save(src, dst):
        c = pltpu.make_async_copy(src, dst, osem.at[len(outs)])
        c.start()
        outs.append(c)

    pump.until(0)
    load(hq, wq, 0).wait()
    for m in range(3):
        def project(i, m=m):
            r = lane(i, 256)
            x = embed(tok[r, :], seg[r, :], table[...]).astype(BF)
            y = dot(x, wq[m * 1024:(m + 1) * 1024, :])
            if m != 1:
                y = y + bias[m // 2:m // 2 + 1, :].astype(F32)
            qkv[m, r, :] = y.astype(BF)
        pump.loop(steps, project, 2)
        save(qkv.at[m], qkv_o.at[m])
    heads = qkv.shape[2] // 128

    def attention(j):
        s, i = j // heads, j % heads
        rows = pl.ds(pl.multiple_of(s * seq, seq), seq)
        cols = lane(i, 128)
        c, t = attend(qkv[0, rows, cols], qkv[1, rows, cols], qkv[2, rows, cols], lengths[s])
        ctx[rows, cols] = c
        for h in range(2):
            totals[pl.ds(s * HEADS + i * 2 + h, 1), :] = t[h]
    pump.loop(n // seq * heads, attention)
    pump.until(1)
    load(ho, wo, 0).wait()
    pump.loop(steps, lambda i: middle_rows(lane(i, 256), tok, seg, table, ctx, wo, bias, normed, inv))
    save(normed, normed_o)
    pump.until(2)
    tiles = [load(h1.at[t], w1.at[t], t) for t in range(4)]
    for t in range(4):
        tiles[t].wait()
        pump.loop(steps, lambda i, t=t: expand_rows(lane(i, 256), t, w1[t], normed, gain, shift, bias1, hidden, slope), 2)
        c = pl.ds(t * 1024, 1024)
        save(hidden.at[:, c], hidden_o.at[:, c])
        save(slope.at[:, c], slope_o.at[:, c])
    pump.until(3)
    for c in outs:
        c.wait()
    if gathers:
        for g in range(4):
            G.sent(g)


def front_call(lengths, tok, seg, table, bias, bias1, gain, shift, weights, seq, gathers):
    n, d = tok.shape
    ff = bias1.shape[1]
    S = jax.ShapeDtypeStruct
    vm = pl.BlockSpec(memory_space=pltpu.VMEM)
    hbm = pl.BlockSpec(memory_space=pl.ANY)
    full = [S((3 * d, d), BF), S((d, d), BF), S((4, d, ff // 4), BF), S((4, ff // 4, d), BF)]
    res = pl.pallas_call(
        functools.partial(front_kernel, seq, gathers),
        in_specs=[pl.BlockSpec(memory_space=pltpu.SMEM)] + [vm] * 7 + [vm if gathers else hbm] * 4,
        out_specs=([hbm] * 4 if gathers else []) + [hbm, vm, hbm, vm, hbm, hbm],
        out_shape=(full if gathers else []) + [S((3, n, d), BF), S((n // seq * HEADS, seq), F32), S((n, d), F32), S((n, 1), F32), S((n, ff), BF), S((n, ff), BF)],
        scratch_shapes=[pltpu.VMEM((3, n, d), BF), pltpu.VMEM((n, d), BF), pltpu.VMEM((n, d), F32), pltpu.VMEM((n, ff), BF), pltpu.VMEM((n, ff), BF),
                        pltpu.VMEM((3 * d, d), BF), pltpu.VMEM((d, d), BF), pltpu.VMEM((4, d, ff // 4), BF),
                        pltpu.SemaphoreType.DMA((4,)), pltpu.SemaphoreType.DMA((12,))] + (sem_shapes(4) if gathers else []),
        compiler_params=pltpu.CompilerParams(vmem_limit_bytes=64 * 1024 * 1024 - 65536, **(dict(collective_id=1, has_side_effects=True) if gathers else {})),
        name="front",
    )(lengths, tok, seg, table, bias, bias1, gain, shift, *weights)
    return tuple(weights) + tuple(res) if not gathers else tuple(res)


def sum_kernel(g_q, g_v, g_bo, g_b1, g_b2, g_gain, g_shift, o_attn, o_b1, o_b2, o_gain, o_shift, mine, core, square, line, ss, rs):
    dp = lax.axis_index("dp")
    tn = lax.axis_index("tensor")
    z, y, x, c = dp // 2, dp % 2, tn // 2, tn % 2
    dev = lambda z, y, x, c: (z * 2 + y, x * 2 + c)
    peers = [dev(z, y, x, 1 - c)]
    peers += [dev(z, (y + k // 2) % 2, (x + k % 2) % 2, c) for k in (1, 2, 3)]
    peers += [dev((z + k) % 4, y, x, c) for k in (1, 2, 3)]
    b = pltpu.get_barrier_semaphore()
    for p in peers:
        pl.semaphore_signal(b, inc=1, device_id=p, device_id_type=MESH)
    mine[0:1, :] = g_q[...]
    mine[1:2, :] = g_v[...]
    mine[2:3, :] = g_bo[...]
    for t in range(4):
        mine[3 + t:4 + t, :] = g_b1[:, t * 1024:(t + 1) * 1024]
    mine[7:8, :] = g_b2[...]
    mine[8:10, :] = g_gain[...]
    mine[10:12, :] = g_shift[...]
    mine[12:16, :] = jnp.zeros((4, 1024), F32)
    pl.semaphore_wait(b, 7)

    def send(k, src, dst, peer):
        return pltpu.make_async_remote_copy(src_ref=src, dst_ref=dst, send_sem=ss.at[k], recv_sem=rs.at[k], device_id=peer, device_id_type=MESH)
    first = send(0, mine, core, peers[0])
    first.start()
    first.wait()
    me = y * 2 + x
    square[me] = mine[...] + core[...]
    copies = [send(k, square.at[me], square.at[me], peers[k]) for k in (1, 2, 3)]
    for a in copies:
        a.start()
    for a in copies:
        a.wait()
    line[z] = (square[0] + square[1]) + (square[2] + square[3])
    copies = [send(3 + k, line.at[z], line.at[z], peers[3 + k]) for k in (1, 2, 3)]
    for a in copies:
        a.start()
    for a in copies:
        a.wait()
    total = (line[0] + line[1]) + (line[2] + line[3])
    o_attn[...] = total[0:3]
    o_b1[...] = total[3:7]
    o_b2[...] = total[7:8]
    o_gain[...] = total[8:10]
    o_shift[...] = total[10:12]


def sum_call(*parts):
    S = jax.ShapeDtypeStruct
    vm = pl.BlockSpec(memory_space=pltpu.VMEM)
    return pl.pallas_call(
        sum_kernel,
        in_specs=[vm] * 7, out_specs=[vm] * 5,
        out_shape=[S((3, 1024), F32), S((4, 1024), F32), S((1, 1024), F32), S((2, 1024), F32), S((2, 1024), F32)],
        scratch_shapes=[pltpu.VMEM((16, 1024), F32), pltpu.VMEM((16, 1024), F32), pltpu.VMEM((4, 16, 1024), F32), pltpu.VMEM((4, 16, 1024), F32),
                        pltpu.SemaphoreType.DMA((7,)), pltpu.SemaphoreType.DMA((7,))],
        compiler_params=pltpu.CompilerParams(collective_id=2, has_side_effects=True),
        name="sum_gradients",
    )(*parts)


def per_device(tokens, segments, lengths, type_table, attn_weight, out_weight, ffn_in_weight, ffn_out_weight, attn_bias,
               ffn_bias_in, ffn_bias_out, norm_gain, norm_shift, cotangent):
    n, d = tokens.shape
    seq = segments.shape[1]
    kernels = lax.axis_size("dp") == 8 and lax.axis_size("tensor") == 4
    if kernels:
        weights = attn_weight.reshape(-1, d), out_weight.reshape(-1, d), ffn_in_weight, ffn_out_weight
    else:
        wq = lax.all_gather(attn_weight, ("dp", "tensor"), axis=0, tiled=True).reshape(-1, d)
        wo = lax.all_gather(out_weight, ("dp", "tensor"), axis=0, tiled=True).reshape(-1, d)
        w1 = lax.all_gather(lax.all_gather(ffn_in_weight, "dp", axis=0, tiled=True), "tensor", axis=1, tiled=True)
        w1 = w1.reshape(d, 4, -1).transpose(1, 0, 2)
        w2 = lax.all_gather(lax.all_gather(ffn_out_weight, "dp", axis=1, tiled=True), "tensor", axis=0, tiled=True).reshape(4, -1, d)
        weights = wq, wo, w1, w2
    wq, wo, w1, w2, qkv, totals, normed, inv, hidden, slope = front_call(
        lengths, tokens, segments.reshape(-1, 1), type_table, attn_bias, ffn_bias_in[None], norm_gain, norm_shift, weights, seq, kernels)
    output, dfirst, dctx, g_bo, g_b1, g_b2, g_gain, g_shift = mlp_call(
        hidden, slope, normed, inv, cotangent, w1, w2, wo, norm_gain, norm_shift, ffn_bias_out[None])
    grad_input, g_q, g_v = back_call(lengths, qkv, dctx, totals, dfirst, wq, seq)
    if kernels:
        g_attn, g_b1, g_b2, g_gain, g_shift = sum_call(g_q, g_v, g_bo, g_b1, g_b2, g_gain, g_shift)
        return output, grad_input, g_attn, g_b1.reshape(-1), g_b2[0], g_gain, g_shift
    g_attn = jnp.concatenate([g_q, g_v, g_bo], axis=0)
    sums = lax.psum((g_attn, g_b1[0], g_b2[0], g_gain, g_shift), ("dp", "tensor"))
    return (output, grad_input) + tuple(sums)


def solution(mesh):
    rows = P(("dp", "tensor"), None)
    flat = P(("dp", "tensor"))
    in_specs = (rows, rows, flat, P(), flat, flat, P("dp", "tensor"), P("tensor", "dp"), P(), P(), P(), P(), P(), rows)
    return jax.shard_map(per_device, mesh=mesh, in_specs=in_specs, out_specs=(rows, rows, P(), P(), P(), P(), P()), check_vma=False)
```
